32 devices in a mesh: depth: 8 (over y, x, core), rays: 4 (over z).
Axes of the slice: x: 2, y: 2, z: 4, core: 2. Of those that a mesh axis runs over, the one named last changes fastest.
Arguments:
- density: float32 [256, 65536], P('depth', 'rays'), may hold values from 0.0001953125 to 0.815625
- radiance: float32 [3, 256, 65536], P(None, 'depth', 'rays'), may hold values from 0 to 1
- target: float32 [3, 65536], P(None, 'rays'), may hold values from 0 to 1
Outputs:
- grad_density: float32 [256, 65536], P('depth', 'rays')
- loss_mean: float32 [], replicated
The draws below stay inside these ranges and needn't reach their ends.
All inputs are finite; a program needn't handle non-finite values.
Results may differ from the reference program's by a relative error of at most 0.0003.
Values sent between devices are 32-bit elements; how exact they have to be, the bound alone decides.
A program may use at most 128 MiB of HBM per device.

```python
import math
import jax
import jax.numpy as jnp
from jax import lax

POINT_COUNT = 256
RAYS = 65536


def draw_density(key, part):
    base_key = jax.random.fold_in(key, 7301)
    first_key, second_key, third_key, fourth_key = jax.random.split(base_key, 4)
    starting_shift_amount = jnp.exp(jax.random.uniform(first_key, (POINT_COUNT, RAYS), jnp.float32, math.log(0.1), math.log(2.0)))
    multiplier_coefficient = jnp.exp(jax.random.uniform(second_key, (1, RAYS), jnp.float32, math.log(0.5), math.log(2.0)))
    location_numbers = jax.random.randint(third_key, (2, RAYS), 0, POINT_COUNT)
    elevation_levels = jax.random.uniform(fourth_key, (2, RAYS), jnp.float32, 0.15, 0.4)
    vertical_element = jnp.arange(POINT_COUNT, dtype=jnp.int32)[:, None]
    packet_clusters = jnp.where(vertical_element == location_numbers[0:1], elevation_levels[0:1], 0.0) + jnp.where(vertical_element == location_numbers[1:2], elevation_levels[1:2], 0.0)
    return (starting_shift_amount * multiplier_coefficient / POINT_COUNT + packet_clusters).astype(jnp.float32)


def shard_levels(stream_key, dims, pieces, smallest, high):
    def one(dim, blocks):
        draws = jax.random.uniform(jax.random.fold_in(jax.random.fold_in(stream_key, 6), dim), (blocks,), jnp.float32, smallest / len(pieces), high / len(pieces))
        return jnp.repeat(jnp.exp(draws), dims[dim] // blocks).reshape((-1,) + (1,) * (len(dims) - dim - 1))

    gain = one(*pieces[0])
    for cut in pieces[1:]:
        gain = gain * one(*cut)
    return gain


def setup_inputs(seed: int = 0) -> dict:
    keys = jax.random.split(jax.random.key(seed), 4)
    density = draw_density(jax.random.fold_in(keys[3], 71), 0)
    radiance = jnp.clip(1.0 * jax.random.uniform(keys[1], (3, POINT_COUNT, RAYS), jnp.float32) ** shard_levels(keys[1], (3, POINT_COUNT, RAYS), ((1, 8), (2, 4)), -0.2, 0.2), 0.0, 1.0)
    target = jnp.clip(1.0 * jax.random.uniform(keys[2], (3, RAYS), jnp.float32) ** shard_levels(keys[2], (3, RAYS), ((1, 4),), -0.2, 0.2), 0.0, 1.0)
    return dict(density=density, radiance=radiance, target=target)


def render_block(density, radiance, target):
    width = density.shape[1]
    zero_row = jnp.zeros((1, width), jnp.float32)
    zero_plane = jnp.zeros((3, 1, width), jnp.float32)
    sample_density = 0.5 * (density + jnp.concatenate([density[1:], zero_row], axis=0))
    sample_color = 0.5 * (radiance + jnp.concatenate([radiance[:, 1:], zero_plane], axis=1))
    running = jnp.cumsum(sample_density, axis=0)
    optical = jnp.concatenate([zero_row, running[:-1]], axis=0)
    transmit = jnp.exp(-optical)
    weight = transmit * (-jnp.expm1(-sample_density))
    emitted = weight[None] * sample_color
    prefix = jnp.cumsum(emitted, axis=1)
    pixel_color = prefix[:, -1]
    remaining = pixel_color[:, None, :] - prefix
    residual_grad = 2.0 * (pixel_color - target)
    transmit_next = transmit * jnp.exp(-sample_density)
    bracket = transmit_next[None] * sample_color - remaining
    sample_grad = jnp.sum(residual_grad[:, None, :] * bracket, axis=0)
    shifted = jnp.concatenate([zero_row, sample_grad[:-1]], axis=0)
    grad_block = 0.5 * (sample_grad + shifted)
    error_term = pixel_color - target
    return grad_block, jnp.sum(error_term * error_term)


def reference(density, radiance, target):
    block_rays = math.gcd(RAYS, 4096)
    block_count = RAYS // block_rays

    def render_one(block_index):
        start = (block_index * block_rays).astype(jnp.int32)
        part_density = lax.dynamic_slice_in_dim(density, start, block_rays, 1)
        part_radiance = lax.dynamic_slice_in_dim(radiance, start, block_rays, 2)
        part_target = lax.dynamic_slice_in_dim(target, start, block_rays, 1)
        return render_block(part_density, part_radiance, part_target)

    block_grads, losses = lax.map(render_one, jnp.arange(block_count, dtype=jnp.int32))
    grad_density = jnp.moveaxis(block_grads, 0, 1).reshape(POINT_COUNT, RAYS)
    loss_mean = jnp.sum(losses) / (3.0 * RAYS)
    return grad_density, loss_mean
```

```python
import functools
import math

import jax
import jax.numpy as jnp
from jax import lax
from jax.experimental import pallas as pl
from jax.experimental.pallas import tpu as pltpu
from jax.sharding import PartitionSpec as P

MESH = pl.DeviceIdType.MESH
SUB, LANE = 8, 128
CHANNELS = 3
HALF_LOG2E = 0.5 * math.log2(math.e)


def kernel(sizes, density_hbm, radiance_hbm, target_ref, grad, loss_ref,
           dens, rad, trans, next_out, prev_out, next_in, prev_in,
           summary, gathered, before, answer, answers, loss_z, loss_sum, loss_d,
           load_sem, halo_send, halo_recv, sum_send, sum_recv,
           ans_send, ans_recv, z_send, z_recv, d_send, d_recv):
    slabs, tiles_z, rows, tiles = sizes
    bands = rows // SUB
    share = tiles // slabs
    group = min(SUB, share)
    plane = rows * tiles
    me = lax.axis_index("depth")
    my_z = lax.axis_index("rays")

    order = [0] + ([bands - 1] if bands > 1 else []) + list(range(1, bands - 1))
    span = tiles * SUB

    def load(band):
        copies = [pltpu.make_async_copy(
            density_hbm.at[pl.ds(band * span, span)], dens.at[pl.ds(band * span, span)],
            load_sem.at[0, band])]
        for c in range(CHANNELS):
            piece = pl.ds(c * plane + band * span, span)
            copies.append(pltpu.make_async_copy(
                radiance_hbm.at[piece], rad.at[piece], load_sem.at[1 + c, band]))
        return copies

    for band in order:
        for copy in load(band):
            copy.start()

    barrier = pltpu.get_barrier_semaphore()
    for k in range(1, slabs):
        pl.semaphore_signal(barrier, inc=1, device_id={"depth": lax.rem(me + k, slabs)}, device_id_type=MESH)
    for k in range(1, tiles_z):
        pl.semaphore_signal(barrier, inc=1, device_id={"rays": lax.rem(my_z + k, tiles_z)}, device_id_type=MESH)

    def row(ref, start, first, count, r):
        base = start + ((r // SUB) * tiles + first) * SUB + r % SUB
        return ref[pl.ds(base, count, stride=SUB), :]

    for band in order[:2]:
        for copy in load(band):
            copy.wait()

    @pl.loop(0, tiles // group)
    def _(b):
        first = b * group
        chunk = first // share
        inner = pl.ds(first - chunk * share, group)
        next_out[chunk, 0, inner] = row(dens, 0, first, group, 0)
        for c in range(CHANNELS):
            next_out[chunk, 1 + c, inner] = row(rad, c * plane, first, group, 0)
            prev_out[chunk, c, inner] = row(rad, c * plane, first, group, rows - 1)

    pl.semaphore_wait(barrier, slabs - 1 + tiles_z - 1)

    def halo(direction, chunk):
        if direction == 0:
            return pltpu.make_async_remote_copy(
                src_ref=next_out.at[chunk], dst_ref=next_in.at[chunk],
                send_sem=halo_send.at[0, chunk], recv_sem=halo_recv.at[0, chunk],
                device_id={"depth": lax.rem(me + slabs - 1, slabs)}, device_id_type=MESH)
        return pltpu.make_async_remote_copy(
            src_ref=prev_out.at[chunk], dst_ref=prev_in.at[chunk],
            send_sem=halo_send.at[1, chunk], recv_sem=halo_recv.at[1, chunk],
            device_id={"depth": lax.rem(me + 1, slabs)}, device_id_type=MESH)

    @pl.when(me > 0)
    def _():
        for k in range(slabs):
            halo(0, lax.rem(me + k, slabs)).start()

    @pl.when(me < slabs - 1)
    def _():
        for k in range(slabs):
            halo(1, lax.rem(me + slabs - k, slabs)).start()

    @pl.when(me == slabs - 1)
    def _():
        next_in[...] = jnp.zeros_like(next_in)

    @pl.when(me == 0)
    def _():
        prev_in[...] = jnp.zeros_like(prev_in)

    for band in order[2:]:
        for copy in load(band):
            copy.wait()

    def send_summary(q):
        return pltpu.make_async_remote_copy(
            src_ref=summary.at[q], dst_ref=gathered.at[me],
            send_sem=sum_send.at[q], recv_sem=sum_recv.at[me],
            device_id={"depth": q}, device_id_type=MESH)

    def recv_summary(q):
        return pltpu.make_async_remote_copy(
            src_ref=summary.at[q], dst_ref=gathered.at[q],
            send_sem=sum_send.at[q], recv_sem=sum_recv.at[q],
            device_id={"depth": q}, device_id_type=MESH)

    def forward(p):
        @pl.when(me < slabs - 1)
        def _():
            halo(0, p).wait_recv()

        @pl.loop(0, share // group)
        def _(b):
            inner = pl.ds(b * group, group)
            first = p * share + b * group
            d_now = row(dens, 0, first, group, 0)
            c_now = [row(rad, c * plane, first, group, 0) for c in range(CHANNELS)]
            depth = jnp.zeros((group, LANE), jnp.float32)
            t_now = jnp.ones((group, LANE), jnp.float32)
            color = [jnp.zeros((group, LANE), jnp.float32) for _ in range(CHANNELS)]
            for r in range(rows):
                if r + 1 < rows:
                    d_next = row(dens, 0, first, group, r + 1)
                    c_next = [row(rad, c * plane, first, group, r + 1) for c in range(CHANNELS)]
                else:
                    d_next = next_in[p, 0, inner]
                    c_next = [next_in[p, 1 + c, inner] for c in range(CHANNELS)]
                depth = depth + (d_now + d_next)
                t_next = jnp.exp2(depth * (-HALF_LOG2E))
                weight = t_now - t_next
                color = [color[c] + weight * (c_now[c] + c_next[c]) for c in range(CHANNELS)]
                trans[r, pl.ds(first, group)] = t_next
                d_now, c_now, t_now = d_next, c_next, t_next
            summary[p, 0, inner] = depth
            for c in range(CHANNELS):
                summary[p, 1 + c, inner] = color[c]

    @pl.loop(1, slabs)
    def _(k):
        p = lax.rem(me + k, slabs)
        forward(p)
        send_summary(p).start()

    forward(me)
    gathered[me] = summary[me]
    @pl.loop(1, slabs)
    def _(k):
        recv_summary(lax.rem(me + slabs - k, slabs)).wait_recv()

    start = jnp.zeros((share, LANE), jnp.float32)
    pixel = [jnp.zeros((share, LANE), jnp.float32) for _ in range(CHANNELS)]
    for q in range(slabs):
        offset = jnp.exp2(start * (-HALF_LOG2E))
        answer[q, 0] = 0.25 * offset
        half = 0.5 * offset
        for c in range(CHANNELS):
            before[q, c] = pixel[c]
            pixel[c] = pixel[c] + half * gathered[q, 1 + c]
        start = start + gathered[q, 0]

    residual, loss = [], jnp.zeros((share, LANE), jnp.float32)
    for c in range(CHANNELS):
        wanted = jnp.concatenate(
            [target_ref[c:c + 1, pl.ds(pl.multiple_of((me * share + t) * LANE, LANE), LANE)] for t in range(share)], axis=0)
        error = pixel[c] - wanted
        residual.append(2.0 * error)
        loss = loss + error * error

    def send_answer(q):
        return pltpu.make_async_remote_copy(
            src_ref=answer.at[q], dst_ref=answers.at[me],
            send_sem=ans_send.at[q], recv_sem=ans_recv.at[me],
            device_id={"depth": q}, device_id_type=MESH)

    def recv_answer(q):
        return pltpu.make_async_remote_copy(
            src_ref=answer.at[q], dst_ref=answers.at[q],
            send_sem=ans_send.at[q], recv_sem=ans_recv.at[q],
            device_id={"depth": q}, device_id_type=MESH)

    for k in list(range(1, slabs)) + [0]:
        q = lax.rem(me + k, slabs)
        behind = residual[0] * (pixel[0] - before[q, 0])
        for c in range(1, CHANNELS):
            behind = behind + residual[c] * (pixel[c] - before[q, c])
        answer[q, 1] = behind
        for c in range(CHANNELS):
            answer[q, 2 + c] = residual[c]
        if k:
            send_answer(q).start()
        else:
            answers[me] = answer[me]

    loss_z[my_z] = loss

    def z_copy(z, slot):
        return pltpu.make_async_remote_copy(
            src_ref=loss_z.at[my_z], dst_ref=loss_z.at[slot],
            send_sem=z_send.at[z], recv_sem=z_recv.at[slot],
            device_id={"rays": z}, device_id_type=MESH)

    def d_copy(q, slot):
        return pltpu.make_async_remote_copy(
            src_ref=loss_sum, dst_ref=loss_d.at[slot],
            send_sem=d_send.at[q], recv_sem=d_recv.at[slot],
            device_id={"depth": q}, device_id_type=MESH)

    for k in range(1, tiles_z):
        z_copy(lax.rem(my_z + k, tiles_z), my_z).start()

    def backward(p):
        @pl.when(me > 0)
        def _():
            halo(1, p).wait_recv()

        @pl.loop(0, share // group)
        def _(b):
            inner = pl.ds(b * group, group)
            first = p * share + b * group
            scale = answers[p, 0, inner]
            behind = answers[p, 1, inner]
            res = [answers[p, 2 + c, inner] for c in range(CHANNELS)]

            def mix(values):
                total = res[0] * values[0]
                for c in range(1, CHANNELS):
                    total = total + res[c] * values[c]
                return total

            v_now = mix([row(rad, c * plane, first, group, 0) for c in range(CHANNELS)])
            a_prev = v_now + mix([prev_in[p, c, inner] for c in range(CHANNELS)])
            a_prev = jnp.where(me == 0, 2.0 * behind, a_prev)
            run = None
            t_now = None
            for r in range(rows):
                if r + 1 < rows:
                    v_next = mix([row(rad, c * plane, first, group, r + 1) for c in range(CHANNELS)])
                else:
                    v_next = mix([next_in[p, 1 + c, inner] for c in range(CHANNELS)])
                u = v_now + v_next
                a = u if r == 0 else t_now * u + run
                t_now = trans[r, pl.ds(first, group)]
                run = a - t_now * u
                base = ((r // SUB) * tiles + first) * SUB + r % SUB
                grad[pl.ds(base, group, stride=SUB), :] = scale * (a + a_prev) - behind
                a_prev, v_now = a, v_next
    backward(me)
    half_way = max(1, slabs // 2)

    @pl.loop(1, half_way)
    def _(k):
        p = lax.rem(me + slabs - k, slabs)
        recv_answer(p).wait_recv()
        backward(p)

    for k in range(1, tiles_z):
        z = lax.rem(my_z + k, tiles_z)
        z_copy(z, z).wait_recv()
    total = loss_z[0]
    for z in range(1, tiles_z):
        total = total + loss_z[z]
    loss_sum[...] = total
    loss_d[me] = total
    for k in range(1, slabs):
        d_copy(lax.rem(me + k, slabs), me).start()

    @pl.loop(half_way, slabs)
    def _(k):
        p = lax.rem(me + slabs - k, slabs)
        recv_answer(p).wait_recv()
        backward(p)

    for k in range(1, slabs):
        q = lax.rem(me + k, slabs)
        d_copy(q, q).wait_recv()
    total = loss_d[0]
    for q in range(1, slabs):
        total = total + loss_d[q]
    loss_ref[0, 0] = jnp.sum(total) / (float(CHANNELS) * tiles_z * tiles * LANE)

    @pl.when(me > 0)
    def _():
        for p in range(slabs):
            halo(0, p).wait_send()

    @pl.when(me < slabs - 1)
    def _():
        for p in range(slabs):
            halo(1, p).wait_send()

    for k in range(1, slabs):
        q = lax.rem(me + k, slabs)
        send_summary(q).wait_send()
        send_answer(q).wait_send()
        d_copy(q, me).wait_send()
    for k in range(1, tiles_z):
        z_copy(lax.rem(my_z + k, tiles_z), my_z).wait_send()


def flat(x):
    lead, (rows, rays) = x.shape[:-2], x.shape[-2:]
    x = x.reshape(-1, rows // SUB, SUB, rays // LANE, LANE)
    return x.swapaxes(2, 3).reshape(-1, LANE)


def on_device(slabs, tiles_z, density, radiance, target):
    rows, rays = density.shape
    tiles = rays // LANE
    share = tiles // slabs
    vmem = lambda *shape: pltpu.VMEM(shape, jnp.float32)
    dma = lambda *shape: pltpu.SemaphoreType.DMA(shape)
    stay = pl.BlockSpec(memory_space=pltpu.HBM)
    bands = rows // SUB
    grad, loss = pl.pallas_call(
        functools.partial(kernel, (slabs, tiles_z, rows, tiles)),
        out_shape=(
            jax.ShapeDtypeStruct((rows * tiles, LANE), jnp.float32),
            jax.ShapeDtypeStruct((1, 1), jnp.float32),
        ),
        in_specs=[stay, stay, pl.BlockSpec(memory_space=pltpu.VMEM)],
        out_specs=(pl.BlockSpec(memory_space=pltpu.VMEM), pl.BlockSpec(memory_space=pltpu.SMEM)),
        scratch_shapes=[
            vmem(rows * tiles, LANE),
            vmem(CHANNELS * rows * tiles, LANE),
            vmem(rows, tiles, LANE),
            vmem(slabs, 1 + CHANNELS, share, LANE),
            vmem(slabs, CHANNELS, share, LANE),
            vmem(slabs, 1 + CHANNELS, share, LANE),
            vmem(slabs, CHANNELS, share, LANE),
            vmem(slabs, 1 + CHANNELS, share, LANE),
            vmem(slabs, 1 + CHANNELS, share, LANE),
            vmem(slabs, CHANNELS, share, LANE),
            vmem(slabs, 2 + CHANNELS, share, LANE),
            vmem(slabs, 2 + CHANNELS, share, LANE),
            vmem(tiles_z, share, LANE),
            vmem(share, LANE),
            vmem(slabs, share, LANE),
            dma(1 + CHANNELS, bands),
            dma(2, slabs), dma(2, slabs),
            dma(slabs), dma(slabs), dma(slabs), dma(slabs),
            dma(tiles_z), dma(tiles_z), dma(slabs), dma(slabs),
        ],
        compiler_params=pltpu.CompilerParams(
            collective_id=0, has_side_effects=True, vmem_limit_bytes=58 * 1024 * 1024),
    )(flat(density), flat(radiance), target)
    grad = grad.reshape(bands, tiles, SUB, LANE).swapaxes(1, 2).reshape(rows, rays)
    return grad, loss.reshape(())


def solution(mesh):
    in_specs = (P("depth", "rays"), P(None, "depth", "rays"), P(None, "rays"))
    out_specs = (P("depth", "rays"), P())
    body = functools.partial(on_device, mesh.shape["depth"], mesh.shape["rays"])
    return jax.shard_map(body, mesh=mesh, in_specs=in_specs, out_specs=out_specs, check_vma=False)
```

```python
import functools
import math

import jax
import jax.numpy as jnp
from jax import lax
from jax.experimental import pallas as pl
from jax.experimental.pallas import tpu as pltpu
from jax.sharding import PartitionSpec as P

MESH = pl.DeviceIdType.MESH
SUB, LANE = 8, 128
CHANNELS = 3
HALF_LOG2E = 0.5 * math.log2(math.e)


def kernel(sizes, density_hbm, radiance_hbm, target_hbm, grad, loss_ref,
           dens, rad, trans, next_out, prev_out, next_in, prev_in,
           summary, gathered, before, answer, answers, wanted, loss_all,
           load_sem, target_sem, halo_send, halo_recv, sum_send, sum_recv,
           ans_send, ans_recv, loss_send, loss_recv):
    slabs, tiles_z, rows, tiles = sizes
    bands = rows // SUB
    share = tiles // slabs
    group = min(SUB, share)
    plane = rows * tiles
    me = lax.axis_index("depth")
    my_z = lax.axis_index("rays")
    devices = slabs * tiles_z
    my_id = me * tiles_z + my_z
    paired = slabs & (slabs - 1) == 0

    def partner(who, k, back=False):
        if not paired:
            return lax.rem(who + (slabs - k if back else k), slabs)
        found, bit = 0, 1
        while bit < slabs:
            found = found + ((who // bit + k // bit) % 2) * bit
            bit *= 2
        return found

    order = [0] + ([bands - 1] if bands > 1 else []) + list(range(1, bands - 1))
    span = tiles * SUB

    def load(band):
        copies = [pltpu.make_async_copy(
            density_hbm.at[pl.ds(band * span, span)], dens.at[pl.ds(band * span, span)],
            load_sem.at[0, band])]
        for c in range(CHANNELS):
            piece = pl.ds(c * plane + band * span, span)
            copies.append(pltpu.make_async_copy(
                radiance_hbm.at[piece], rad.at[piece], load_sem.at[1 + c, band]))
        return copies

    for band in order:
        for copy in load(band):
            copy.start()

    target_copy = pltpu.make_async_copy(
        target_hbm.at[:, pl.ds(pl.multiple_of(me * share * LANE, LANE), share * LANE)], wanted, target_sem)
    target_copy.start()

    barrier = pltpu.get_barrier_semaphore()
    for k in range(1, slabs):
        pl.semaphore_signal(barrier, inc=1, device_id={"depth": lax.rem(me + k, slabs)}, device_id_type=MESH)
    for k in range(1, tiles_z):
        pl.semaphore_signal(barrier, inc=1, device_id={"rays": lax.rem(my_z + k, tiles_z)}, device_id_type=MESH)

    def row(ref, start, first, count, r):
        base = start + ((r // SUB) * tiles + first) * SUB + r % SUB
        return ref[pl.ds(base, count, stride=SUB), :]

    for band in order[:2]:
        for copy in load(band):
            copy.wait()

    @pl.loop(0, tiles // group)
    def _(b):
        first = b * group
        chunk = first // share
        inner = pl.ds(first - chunk * share, group)
        next_out[chunk, 0, inner] = row(dens, 0, first, group, 0)
        for c in range(CHANNELS):
            next_out[chunk, 1 + c, inner] = row(rad, c * plane, first, group, 0)
            prev_out[chunk, c, inner] = row(rad, c * plane, first, group, rows - 1)

    pl.semaphore_wait(barrier, slabs - 1 + tiles_z - 1)

    def halo(direction, chunk):
        if direction == 0:
            return pltpu.make_async_remote_copy(
                src_ref=next_out.at[chunk], dst_ref=next_in.at[chunk],
                send_sem=halo_send.at[0, chunk], recv_sem=halo_recv.at[0, chunk],
                device_id={"depth": lax.rem(me + slabs - 1, slabs)}, device_id_type=MESH)
        return pltpu.make_async_remote_copy(
            src_ref=prev_out.at[chunk], dst_ref=prev_in.at[chunk],
            send_sem=halo_send.at[1, chunk], recv_sem=halo_recv.at[1, chunk],
            device_id={"depth": lax.rem(me + 1, slabs)}, device_id_type=MESH)

    @pl.when(me > 0)
    def _():
        for k in range(slabs - 1, -1, -1):
            halo(0, partner(me - 1, k)).start()

    @pl.when(me == slabs - 1)
    def _():
        next_in[...] = jnp.zeros_like(next_in)

    @pl.when(me == 0)
    def _():
        prev_in[...] = jnp.zeros_like(prev_in)

    for band in order[2:]:
        for copy in load(band):
            copy.wait()

    def send_summary(q):
        return pltpu.make_async_remote_copy(
            src_ref=summary.at[q], dst_ref=gathered.at[me],
            send_sem=sum_send.at[q], recv_sem=sum_recv.at[me],
            device_id={"depth": q}, device_id_type=MESH)

    def recv_summary(q):
        return pltpu.make_async_remote_copy(
            src_ref=summary.at[q], dst_ref=gathered.at[q],
            send_sem=sum_send.at[q], recv_sem=sum_recv.at[q],
            device_id={"depth": q}, device_id_type=MESH)

    def forward(p):
        @pl.when(me < slabs - 1)
        def _():
            halo(0, p).wait_recv()

        @pl.loop(0, share // group)
        def _(b):
            inner = pl.ds(b * group, group)
            first = p * share + b * group
            d_now = row(dens, 0, first, group, 0)
            c_now = [row(rad, c * plane, first, group, 0) for c in range(CHANNELS)]
            depth = jnp.zeros((group, LANE), jnp.float32)
            t_now = jnp.ones((group, LANE), jnp.float32)
            color = [jnp.zeros((group, LANE), jnp.float32) for _ in range(CHANNELS)]
            for r in range(rows):
                if r + 1 < rows:
                    d_next = row(dens, 0, first, group, r + 1)
                    c_next = [row(rad, c * plane, first, group, r + 1) for c in range(CHANNELS)]
                else:
                    d_next = next_in[p, 0, inner]
                    c_next = [next_in[p, 1 + c, inner] for c in range(CHANNELS)]
                depth = depth + (d_now + d_next)
                t_next = jnp.exp2(depth * (-HALF_LOG2E))
                weight = t_now - t_next
                color = [color[c] + weight * (c_now[c] + c_next[c]) for c in range(CHANNELS)]
                trans[r, pl.ds(first, group)] = t_next
                d_now, c_now, t_now = d_next, c_next, t_next
            summary[p, 0, inner] = depth
            for c in range(CHANNELS):
                summary[p, 1 + c, inner] = color[c]

    @pl.loop(1, slabs)
    def _(i):
        p = partner(me, slabs - i)
        forward(p)
        send_summary(p).start()

    @pl.when(me < slabs - 1)
    def _():
        for k in range(slabs):
            halo(1, partner(me + 1, k)).start()

    forward(me)
    gathered[me] = summary[me]
    target_copy.wait()

    @pl.loop(1, slabs)
    def _(k):
        recv_summary(partner(me, k, True)).wait_recv()

    start = jnp.zeros((share, LANE), jnp.float32)
    pixel = [jnp.zeros((share, LANE), jnp.float32) for _ in range(CHANNELS)]
    for q in range(slabs):
        offset = jnp.exp2(start * (-HALF_LOG2E))
        answer[q, 0] = 0.25 * offset
        half = 0.5 * offset
        for c in range(CHANNELS):
            before[q, c] = pixel[c]
            pixel[c] = pixel[c] + half * gathered[q, 1 + c]
        start = start + gathered[q, 0]

    residual, loss = [], jnp.zeros((share, LANE), jnp.float32)
    for c in range(CHANNELS):
        goal = jnp.concatenate(
            [wanted[c:c + 1, t * LANE:(t + 1) * LANE] for t in range(share)], axis=0)
        error = pixel[c] - goal
        residual.append(2.0 * error)
        loss = loss + error * error

    loss_all[my_id] = jnp.sum(loss, axis=0, keepdims=True)

    def loss_copy(other, slot):
        return pltpu.make_async_remote_copy(
            src_ref=loss_all.at[my_id], dst_ref=loss_all.at[slot],
            send_sem=loss_send.at[other], recv_sem=loss_recv.at[slot],
            device_id={"depth": other // tiles_z, "rays": lax.rem(other, tiles_z)}, device_id_type=MESH)

    @pl.loop(1, devices)
    def _(k):
        loss_copy(lax.rem(my_id + k, devices), my_id).start()

    def send_answer(q):
        return pltpu.make_async_remote_copy(
            src_ref=answer.at[q], dst_ref=answers.at[me],
            send_sem=ans_send.at[q], recv_sem=ans_recv.at[me],
            device_id={"depth": q}, device_id_type=MESH)

    def recv_answer(q):
        return pltpu.make_async_remote_copy(
            src_ref=answer.at[q], dst_ref=answers.at[q],
            send_sem=ans_send.at[q], recv_sem=ans_recv.at[q],
            device_id={"depth": q}, device_id_type=MESH)

    for k in range(slabs - 1, -1, -1):
        q = partner(me, k)
        behind = residual[0] * (pixel[0] - before[q, 0])
        for c in range(1, CHANNELS):
            behind = behind + residual[c] * (pixel[c] - before[q, c])
        answer[q, 1] = behind
        for c in range(CHANNELS):
            answer[q, 2 + c] = residual[c]
        if k:
            send_answer(q).start()
        else:
            answers[me] = answer[me]

    def backward(p):
        @pl.when(me > 0)
        def _():
            halo(1, p).wait_recv()

        @pl.loop(0, share // group)
        def _(b):
            inner = pl.ds(b * group, group)
            first = p * share + b * group
            scale = answers[p, 0, inner]
            behind = answers[p, 1, inner]
            res = [answers[p, 2 + c, inner] for c in range(CHANNELS)]

            def mix(values):
                total = res[0] * values[0]
                for c in range(1, CHANNELS):
                    total = total + res[c] * values[c]
                return total

            v_now = mix([row(rad, c * plane, first, group, 0) for c in range(CHANNELS)])
            a_prev = v_now + mix([prev_in[p, c, inner] for c in range(CHANNELS)])
            a_prev = jnp.where(me == 0, 2.0 * behind, a_prev)
            run = None
            t_now = None
            for r in range(rows):
                if r + 1 < rows:
                    v_next = mix([row(rad, c * plane, first, group, r + 1) for c in range(CHANNELS)])
                else:
                    v_next = mix([next_in[p, 1 + c, inner] for c in range(CHANNELS)])
                u = v_now + v_next
                a = u if r == 0 else t_now * u + run
                t_now = trans[r, pl.ds(first, group)]
                run = a - t_now * u
                base = ((r // SUB) * tiles + first) * SUB + r % SUB
                grad[pl.ds(base, group, stride=SUB), :] = scale * (a + a_prev) - behind
                a_prev, v_now = a, v_next
    backward(me)

    def finish(k):
        p = partner(me, k, True)
        recv_answer(p).wait_recv()
        backward(p)

    if slabs > 1:
        finish(1)

    @pl.loop(1, slabs - 1)
    def _(i):
        finish(slabs - i)

    @pl.loop(1, devices)
    def _(k):
        other = lax.rem(my_id + k, devices)
        loss_copy(other, other).wait_recv()
    total = loss_all[0]
    for other in range(1, devices):
        total = total + loss_all[other]
    loss_ref[0, 0] = jnp.sum(total) / (float(CHANNELS) * tiles_z * tiles * LANE)

    @pl.when(me > 0)
    def _():
        for p in range(slabs):
            halo(0, p).wait_send()

    @pl.when(me < slabs - 1)
    def _():
        for p in range(slabs):
            halo(1, p).wait_send()

    for k in range(1, slabs):
        q = lax.rem(me + k, slabs)
        send_summary(q).wait_send()
        send_answer(q).wait_send()

    @pl.loop(1, devices)
    def _(k):
        loss_copy(lax.rem(my_id + k, devices), my_id).wait_send()


def flat(x):
    lead, (rows, rays) = x.shape[:-2], x.shape[-2:]
    x = x.reshape(-1, rows // SUB, SUB, rays // LANE, LANE)
    return x.swapaxes(2, 3).reshape(-1, LANE)


def on_device(slabs, tiles_z, density, radiance, target):
    rows, rays = density.shape
    tiles = rays // LANE
    share = tiles // slabs
    vmem = lambda *shape: pltpu.VMEM(shape, jnp.float32)
    dma = lambda *shape: pltpu.SemaphoreType.DMA(shape)
    stay = pl.BlockSpec(memory_space=pltpu.HBM)
    bands = rows // SUB
    grad, loss = pl.pallas_call(
        functools.partial(kernel, (slabs, tiles_z, rows, tiles)),
        out_shape=(
            jax.ShapeDtypeStruct((rows * tiles, LANE), jnp.float32),
            jax.ShapeDtypeStruct((1, 1), jnp.float32),
        ),
        in_specs=[stay, stay, stay],
        out_specs=(pl.BlockSpec(memory_space=pltpu.VMEM), pl.BlockSpec(memory_space=pltpu.SMEM)),
        scratch_shapes=[
            vmem(rows * tiles, LANE),
            vmem(CHANNELS * rows * tiles, LANE),
            vmem(rows, tiles, LANE),
            vmem(slabs, 1 + CHANNELS, share, LANE),
            vmem(slabs, CHANNELS, share, LANE),
            vmem(slabs, 1 + CHANNELS, share, LANE),
            vmem(slabs, CHANNELS, share, LANE),
            vmem(slabs, 1 + CHANNELS, share, LANE),
            vmem(slabs, 1 + CHANNELS, share, LANE),
            vmem(slabs, CHANNELS, share, LANE),
            vmem(slabs, 2 + CHANNELS, share, LANE),
            vmem(slabs, 2 + CHANNELS, share, LANE),
            vmem(CHANNELS, share * LANE),
            vmem(slabs * tiles_z, 1, LANE),
            dma(1 + CHANNELS, bands), pltpu.SemaphoreType.DMA,
            dma(2, slabs), dma(2, slabs),
            dma(slabs), dma(slabs), dma(slabs), dma(slabs),
            dma(slabs * tiles_z), dma(slabs * tiles_z),
        ],
        compiler_params=pltpu.CompilerParams(
            collective_id=0, has_side_effects=True, vmem_limit_bytes=50 * 1024 * 1024),
    )(flat(density), flat(radiance), pltpu.with_memory_space_constraint(target, pltpu.HBM))
    grad = grad.reshape(bands, tiles, SUB, LANE).swapaxes(1, 2).reshape(rows, rays)
    return grad, loss.reshape(())


def solution(mesh):
    in_specs = (P("depth", "rays"), P(None, "depth", "rays"), P(None, "rays"))
    out_specs = (P("depth", "rays"), P())
    body = functools.partial(on_device, mesh.shape["depth"], mesh.shape["rays"])
    return jax.shard_map(body, mesh=mesh, in_specs=in_specs, out_specs=out_specs, check_vma=False)
```

```python
import functools
import math

import jax
import jax.numpy as jnp
from jax import lax
from jax.experimental import pallas as pl
from jax.experimental.pallas import tpu as pltpu
from jax.sharding import PartitionSpec as P

MESH = pl.DeviceIdType.MESH
SUB, LANE = 8, 128
CHANNELS = 3
HALF_LOG2E = 0.5 * math.log2(math.e)


def kernel(sizes, density_hbm, radiance_hbm, target_hbm, grad, loss_ref,
           dens, rad, trans, next_out, prev_out, next_in, prev_in,
           summary, gathered, before, answer, answers, wanted, loss_all,
           load_sem, target_sem, halo_send, halo_recv, sum_send, sum_recv,
           ans_send, ans_recv, loss_send, loss_recv):
    slabs, tiles_z, rows, tiles = sizes
    bands = rows // SUB
    share = tiles // slabs
    group = min(SUB, share)
    plane = rows * tiles
    me = lax.axis_index("depth")
    my_z = lax.axis_index("rays")
    devices = slabs * tiles_z
    my_id = me * tiles_z + my_z
    paired = slabs & (slabs - 1) == 0

    def partner(who, k, back=False):
        if not paired:
            return lax.rem(who + (slabs - k if back else k), slabs)
        found, bit = 0, 1
        while bit < slabs:
            found = found + ((who // bit + k // bit) % 2) * bit
            bit *= 2
        return found

    order = range(bands)
    span = tiles * SUB

    def load(band):
        copies = [pltpu.make_async_copy(
            density_hbm.at[pl.ds(band * span, span)], dens.at[pl.ds(band * span, span)],
            load_sem.at[0, band])]
        for c in range(CHANNELS):
            piece = pl.ds(c * plane + band * span, span)
            copies.append(pltpu.make_async_copy(
                radiance_hbm.at[piece], rad.at[piece], load_sem.at[1 + c, band]))
        return copies

    for band in order:
        for copy in load(band):
            copy.start()

    target_copy = pltpu.make_async_copy(
        target_hbm.at[:, pl.ds(pl.multiple_of(me * share * LANE, LANE), share * LANE)], wanted, target_sem)
    target_copy.start()

    barrier = pltpu.get_barrier_semaphore()
    for k in range(1, slabs):
        pl.semaphore_signal(barrier, inc=1, device_id={"depth": lax.rem(me + k, slabs)}, device_id_type=MESH)
    for k in range(1, tiles_z):
        pl.semaphore_signal(barrier, inc=1, device_id={"rays": lax.rem(my_z + k, tiles_z)}, device_id_type=MESH)

    def row(ref, start, first, count, r):
        base = start + ((r // SUB) * tiles + first) * SUB + r % SUB
        return ref[pl.ds(base, count, stride=SUB), :]

    for copy in load(0):
        copy.wait()

    @pl.loop(0, tiles // group)
    def _(b):
        first = b * group
        chunk = first // share
        inner = pl.ds(first - chunk * share, group)
        next_out[chunk, 0, inner] = row(dens, 0, first, group, 0)
        for c in range(CHANNELS):
            next_out[chunk, 1 + c, inner] = row(rad, c * plane, first, group, 0)

    pl.semaphore_wait(barrier, slabs - 1 + tiles_z - 1)

    def halo(direction, chunk):
        if direction == 0:
            return pltpu.make_async_remote_copy(
                src_ref=next_out.at[chunk], dst_ref=next_in.at[chunk],
                send_sem=halo_send.at[0, chunk], recv_sem=halo_recv.at[0, chunk],
                device_id={"depth": lax.rem(me + slabs - 1, slabs)}, device_id_type=MESH)
        return pltpu.make_async_remote_copy(
            src_ref=prev_out.at[chunk], dst_ref=prev_in.at[chunk],
            send_sem=halo_send.at[1, chunk], recv_sem=halo_recv.at[1, chunk],
            device_id={"depth": lax.rem(me + 1, slabs)}, device_id_type=MESH)

    @pl.when(me > 0)
    def _():
        for k in range(slabs - 1, -1, -1):
            halo(0, partner(me - 1, k)).start()

    @pl.when(me == slabs - 1)
    def _():
        next_in[...] = jnp.zeros_like(next_in)

    @pl.when(me == 0)
    def _():
        prev_in[...] = jnp.zeros_like(prev_in)

    for band in order[1:]:
        for copy in load(band):
            copy.wait()

    def send_summary(q):
        return pltpu.make_async_remote_copy(
            src_ref=summary.at[q], dst_ref=gathered.at[me],
            send_sem=sum_send.at[q], recv_sem=sum_recv.at[me],
            device_id={"depth": q}, device_id_type=MESH)

    def recv_summary(q):
        return pltpu.make_async_remote_copy(
            src_ref=summary.at[q], dst_ref=gathered.at[q],
            send_sem=sum_send.at[q], recv_sem=sum_recv.at[q],
            device_id={"depth": q}, device_id_type=MESH)

    @pl.loop(0, tiles // group)
    def _(b):
        first = b * group
        p = first // share
        inner = pl.ds(first - p * share, group)
        d_now = row(dens, 0, first, group, 0)
        c_now = [row(rad, c * plane, first, group, 0) for c in range(CHANNELS)]
        depth = jnp.zeros((group, LANE), jnp.float32)
        t_now = jnp.ones((group, LANE), jnp.float32)
        color = [jnp.zeros((group, LANE), jnp.float32) for _ in range(CHANNELS)]
        for r in range(rows - 1):
            d_next = row(dens, 0, first, group, r + 1)
            c_next = [row(rad, c * plane, first, group, r + 1) for c in range(CHANNELS)]
            depth = depth + (d_now + d_next)
            t_next = jnp.exp2(depth * (-HALF_LOG2E))
            weight = t_now - t_next
            color = [color[c] + weight * (c_now[c] + c_next[c]) for c in range(CHANNELS)]
            trans[r, pl.ds(first, group)] = t_next
            d_now, c_now, t_now = d_next, c_next, t_next
        summary[p, 0, inner] = depth + d_now
        for c in range(CHANNELS):
            summary[p, 1 + c, inner] = color[c]
            prev_out[p, c, inner] = c_now[c]

    def forward(p):
        @pl.when(me < slabs - 1)
        def _():
            halo(0, p).wait_recv()

        @pl.loop(0, share // group)
        def _(b):
            inner = pl.ds(b * group, group)
            here = pl.ds(p * share + b * group, group)
            depth = summary[p, 0, inner] + next_in[p, 0, inner]
            t_next = jnp.exp2(depth * (-HALF_LOG2E))
            weight = trans[rows - 2, here] - t_next
            trans[rows - 1, here] = t_next
            summary[p, 0, inner] = depth
            for c in range(CHANNELS):
                summary[p, 1 + c, inner] = summary[p, 1 + c, inner] + weight * (
                    prev_out[p, c, inner] + next_in[p, 1 + c, inner])

    @pl.loop(1, slabs)
    def _(i):
        p = partner(me, slabs - i)
        forward(p)
        send_summary(p).start()

    @pl.when(me < slabs - 1)
    def _():
        for k in range(slabs):
            halo(1, partner(me + 1, k)).start()

    forward(me)
    gathered[me] = summary[me]
    target_copy.wait()

    @pl.loop(1, slabs)
    def _(k):
        recv_summary(partner(me, k, True)).wait_recv()

    start = jnp.zeros((share, LANE), jnp.float32)
    pixel = [jnp.zeros((share, LANE), jnp.float32) for _ in range(CHANNELS)]
    for q in range(slabs):
        offset = jnp.exp2(start * (-HALF_LOG2E))
        answer[q, 0] = 0.25 * offset
        half = 0.5 * offset
        for c in range(CHANNELS):
            before[q, c] = pixel[c]
            pixel[c] = pixel[c] + half * gathered[q, 1 + c]
        start = start + gathered[q, 0]

    residual, loss = [], jnp.zeros((share, LANE), jnp.float32)
    for c in range(CHANNELS):
        goal = jnp.concatenate(
            [wanted[c:c + 1, t * LANE:(t + 1) * LANE] for t in range(share)], axis=0)
        error = pixel[c] - goal
        residual.append(2.0 * error)
        loss = loss + error * error

    loss_all[my_id] = jnp.sum(loss, axis=0, keepdims=True)

    others_z = [lax.rem(my_z + k, tiles_z) for k in range(tiles_z)]

    def loss_copy(piece, depth, z):
        return pltpu.make_async_remote_copy(
            src_ref=loss_all.at[piece], dst_ref=loss_all.at[piece],
            send_sem=loss_send, recv_sem=loss_recv,
            device_id={"depth": depth, "rays": z}, device_id_type=MESH)

    def send_losses():
        for k in range(slabs - 1, -1, -1):
            depth = partner(me, k)
            for z in others_z[::-1]:
                if k or z is not others_z[0]:
                    loss_copy(pl.ds(my_id, 1), depth, z).start()

    def send_answer(q):
        return pltpu.make_async_remote_copy(
            src_ref=answer.at[q], dst_ref=answers.at[me],
            send_sem=ans_send.at[q], recv_sem=ans_recv.at[me],
            device_id={"depth": q}, device_id_type=MESH)

    def recv_answer(q):
        return pltpu.make_async_remote_copy(
            src_ref=answer.at[q], dst_ref=answers.at[q],
            send_sem=ans_send.at[q], recv_sem=ans_recv.at[q],
            device_id={"depth": q}, device_id_type=MESH)

    for k in range(slabs - 1, -1, -1):
        q = partner(me, k)
        behind = residual[0] * (pixel[0] - before[q, 0])
        for c in range(1, CHANNELS):
            behind = behind + residual[c] * (pixel[c] - before[q, c])
        answer[q, 1] = behind
        for c in range(CHANNELS):
            answer[q, 2 + c] = residual[c]
        if k:
            send_answer(q).start()
        if k == max(0, slabs - 2):
            send_losses()
        if not k:
            answers[me] = answer[me]

    def backward(p):
        @pl.when(me > 0)
        def _():
            halo(1, p).wait_recv()

        @pl.loop(0, share // group)
        def _(b):
            inner = pl.ds(b * group, group)
            first = p * share + b * group
            scale = answers[p, 0, inner]
            behind = answers[p, 1, inner]
            res = [answers[p, 2 + c, inner] for c in range(CHANNELS)]

            def mix(values):
                total = res[0] * values[0]
                for c in range(1, CHANNELS):
                    total = total + res[c] * values[c]
                return total

            v_now = mix([row(rad, c * plane, first, group, 0) for c in range(CHANNELS)])
            a_prev = v_now + mix([prev_in[p, c, inner] for c in range(CHANNELS)])
            a_prev = jnp.where(me == 0, 2.0 * behind, a_prev)
            run = None
            t_now = None
            for r in range(rows):
                if r + 1 < rows:
                    v_next = mix([row(rad, c * plane, first, group, r + 1) for c in range(CHANNELS)])
                else:
                    v_next = mix([next_in[p, 1 + c, inner] for c in range(CHANNELS)])
                u = v_now + v_next
                a = u if r == 0 else t_now * u + run
                t_now = trans[r, pl.ds(first, group)]
                run = a - t_now * u
                base = ((r // SUB) * tiles + first) * SUB + r % SUB
                grad[pl.ds(base, group, stride=SUB), :] = scale * (a + a_prev) - behind
                a_prev, v_now = a, v_next
    backward(me)

    def finish(k):
        p = partner(me, k, True)
        recv_answer(p).wait_recv()
        backward(p)

    if slabs > 1:
        finish(1)

    @pl.loop(1, slabs - 1)
    def _(i):
        finish(slabs - i)

    every_other = loss_copy(pl.ds(0, devices - 1), me, my_z)
    every_other.wait_recv()
    total = loss_all[0]
    for other in range(1, devices):
        total = total + loss_all[other]
    loss_ref[0, 0] = jnp.sum(total) / (float(CHANNELS) * tiles_z * tiles * LANE)

    @pl.when(me > 0)
    def _():
        for p in range(slabs):
            halo(0, p).wait_send()

    @pl.when(me < slabs - 1)
    def _():
        for p in range(slabs):
            halo(1, p).wait_send()

    for k in range(1, slabs):
        q = lax.rem(me + k, slabs)
        send_summary(q).wait_send()
        send_answer(q).wait_send()

    every_other.wait_send()


def flat(x):
    lead, (rows, rays) = x.shape[:-2], x.shape[-2:]
    x = x.reshape(-1, rows // SUB, SUB, rays // LANE, LANE)
    return x.swapaxes(2, 3).reshape(-1, LANE)


def on_device(slabs, tiles_z, density, radiance, target):
    rows, rays = density.shape
    tiles = rays // LANE
    share = tiles // slabs
    vmem = lambda *shape: pltpu.VMEM(shape, jnp.float32)
    dma = lambda *shape: pltpu.SemaphoreType.DMA(shape)
    stay = pl.BlockSpec(memory_space=pltpu.HBM)
    bands = rows // SUB
    grad, loss = pl.pallas_call(
        functools.partial(kernel, (slabs, tiles_z, rows, tiles)),
        out_shape=(
            jax.ShapeDtypeStruct((rows * tiles, LANE), jnp.float32),
            jax.ShapeDtypeStruct((1, 1), jnp.float32),
        ),
        in_specs=[stay, stay, stay],
        out_specs=(pl.BlockSpec(memory_space=pltpu.VMEM), pl.BlockSpec(memory_space=pltpu.SMEM)),
        scratch_shapes=[
            vmem(rows * tiles, LANE),
            vmem(CHANNELS * rows * tiles, LANE),
            vmem(rows, tiles, LANE),
            vmem(slabs, 1 + CHANNELS, share, LANE),
            vmem(slabs, CHANNELS, share, LANE),
            vmem(slabs, 1 + CHANNELS, share, LANE),
            vmem(slabs, CHANNELS, share, LANE),
            vmem(slabs, 1 + CHANNELS, share, LANE),
            vmem(slabs, 1 + CHANNELS, share, LANE),
            vmem(slabs, CHANNELS, share, LANE),
            vmem(slabs, 2 + CHANNELS, share, LANE),
            vmem(slabs, 2 + CHANNELS, share, LANE),
            vmem(CHANNELS, share * LANE),
            vmem(slabs * tiles_z, 1, LANE),
            dma(1 + CHANNELS, bands), pltpu.SemaphoreType.DMA,
            dma(2, slabs), dma(2, slabs),
            dma(slabs), dma(slabs), dma(slabs), dma(slabs),
            pltpu.SemaphoreType.DMA, pltpu.SemaphoreType.DMA,
        ],
        compiler_params=pltpu.CompilerParams(
            collective_id=0, has_side_effects=True, vmem_limit_bytes=50 * 1024 * 1024),
    )(flat(density), flat(radiance), pltpu.with_memory_space_constraint(target, pltpu.HBM))
    grad = grad.reshape(bands, tiles, SUB, LANE).swapaxes(1, 2).reshape(rows, rays)
    return grad, loss.reshape(())


def solution(mesh):
    in_specs = (P("depth", "rays"), P(None, "depth", "rays"), P(None, "rays"))
    out_specs = (P("depth", "rays"), P())
    body = functools.partial(on_device, mesh.shape["depth"], mesh.shape["rays"])
    return jax.shard_map(body, mesh=mesh, in_specs=in_specs, out_specs=out_specs, check_vma=False)
```
